32 devices in a mesh: rep: 4 (over x, y), dp: 8 (over z, core).
Axes of the slice: x: 2, y: 2, z: 4, core: 2. Of those that a mesh axis runs over, the one named last changes fastest.
Arguments:
- x: bfloat16 [32, 2048, 640], P(('rep', 'dp')), parts along dimension 0
- dy: bfloat16 [32, 2048, 640], P(('rep', 'dp')), parts along dimension 0
- wq: bfloat16 [2, 640, 1536], P(None, 'dp')
- wk: bfloat16 [2, 640, 128], P(None, 'dp')
- wv: bfloat16 [2, 640, 128], P(None, 'dp')
- wo: bfloat16 [2, 1536, 640], P(None, 'dp')
- w_gate: bfloat16 [2, 640, 1536], P(None, 'dp')
- w_up: bfloat16 [2, 640, 1536], P(None, 'dp')
- w_down: bfloat16 [2, 1536, 640], P(None, 'dp')
- m_wq: float32 [2, 640, 1536], P(None, 'dp')
- m_wk: float32 [2, 640, 128], P(None, 'dp')
- m_wv: float32 [2, 640, 128], P(None, 'dp')
- m_wo: float32 [2, 1536, 640], P(None, 'dp')
- m_w_gate: float32 [2, 640, 1536], P(None, 'dp')
- m_w_up: float32 [2, 640, 1536], P(None, 'dp')
- m_w_down: float32 [2, 1536, 640], P(None, 'dp')
- v_wq: float32 [2, 640, 1536], P(None, 'dp')
- v_wk: float32 [2, 640, 128], P(None, 'dp')
- v_wv: float32 [2, 640, 128], P(None, 'dp')
- v_wo: float32 [2, 1536, 640], P(None, 'dp')
- v_w_gate: float32 [2, 640, 1536], P(None, 'dp')
- v_w_up: float32 [2, 640, 1536], P(None, 'dp')
- v_w_down: float32 [2, 1536, 640], P(None, 'dp')
Outputs:
- output 1: bfloat16 [8, 640, 1536], P('rep', 'dp'), parts along dimension 0
- output 2: bfloat16 [8, 640, 128], P('rep', 'dp'), parts along dimension 0
- output 3: bfloat16 [8, 640, 128], P('rep', 'dp'), parts along dimension 0
- output 4: bfloat16 [8, 1536, 640], P('rep', 'dp'), parts along dimension 0
- output 5: bfloat16 [8, 640, 1536], P('rep', 'dp'), parts along dimension 0
- output 6: bfloat16 [8, 640, 1536], P('rep', 'dp'), parts along dimension 0
- output 7: bfloat16 [8, 1536, 640], P('rep', 'dp'), parts along dimension 0
- output 8: float32 [8, 640, 1536], P('rep', 'dp'), parts along dimension 0
- output 9: float32 [8, 640, 128], P('rep', 'dp'), parts along dimension 0
- output 10: float32 [8, 640, 128], P('rep', 'dp'), parts along dimension 0
- output 11: float32 [8, 1536, 640], P('rep', 'dp'), parts along dimension 0
- output 12: float32 [8, 640, 1536], P('rep', 'dp'), parts along dimension 0
- output 13: float32 [8, 640, 1536], P('rep', 'dp'), parts along dimension 0
- output 14: float32 [8, 1536, 640], P('rep', 'dp'), parts along dimension 0
- output 15: float32 [8, 640, 1536], P('rep', 'dp'), parts along dimension 0
- output 16: float32 [8, 640, 128], P('rep', 'dp'), parts along dimension 0
- output 17: float32 [8, 640, 128], P('rep', 'dp'), parts along dimension 0
- output 18: float32 [8, 1536, 640], P('rep', 'dp'), parts along dimension 0
- output 19: float32 [8, 640, 1536], P('rep', 'dp'), parts along dimension 0
- output 20: float32 [8, 640, 1536], P('rep', 'dp'), parts along dimension 0
- output 21: float32 [8, 1536, 640], P('rep', 'dp'), parts along dimension 0
There are 4 independent parts. The reference program is written for one: setup_inputs(seed, part) draws one part's arguments, and reference() takes and returns one part's arrays. A program takes and returns all parts, laid end to end along the dimension named above; an argument that names none is the same for every part.
All inputs are finite; a program needn't handle non-finite values.
Results may differ from the reference program's by a relative error of at most 0.026.
Values are sent between devices in bfloat16 or wider.
A program may use at most 2 GiB of HBM per device.

```python
import jax
import jax.numpy as jnp
from jax import lax

SEQUENCES = 8
TOKENS = 2048
D = 640
HEADS = 12
KV_HEADS = 1
HEAD = 128
FF = 1536
LAYERS = 2
THETA = 10000
NAMES = ("wq", "wk", "wv", "wo", "w_gate", "w_up", "w_down")
SHAPES = {
    "wq": (LAYERS, D, HEADS * HEAD),
    "wk": (LAYERS, D, KV_HEADS * HEAD),
    "wv": (LAYERS, D, KV_HEADS * HEAD),
    "wo": (LAYERS, HEADS * HEAD, D),
    "w_gate": (LAYERS, D, FF),
    "w_up": (LAYERS, D, FF),
    "w_down": (LAYERS, FF, D),
}


def bump(key, n, height):
    away = (jnp.arange(n, dtype=jnp.int32) - jax.random.randint(key, (), 0, n, jnp.int32)) % n
    return jnp.where(away < n // 8, height, 1.0)


def together(key, own, strength):
    shared = jax.random.normal(key, own.shape[1:], jnp.float32)
    return (own + strength * shared) * lax.rsqrt(1 + strength * strength)


def setup_inputs(seed: int = 0, part: int = 0) -> dict:
    kx, kdy, ka, kb, kz, kf, kh, kl, *keys = jax.random.split(jax.random.key(seed), 8 + 3 * len(NAMES))
    kx, kdy, ka, kb = (jax.random.fold_in(k, part) for k in (kx, kdy, ka, kb))
    kw, km, kv = (keys[i::3] for i in range(3))
    shape = (SEQUENCES, TOKENS, D)
    much_x, much_dy = jax.random.uniform(kz, (2,), jnp.float32, 0.0, 1.0)
    loud = 2.0 ** jax.random.uniform(jax.random.fold_in(kz, 1), (), jnp.float32, -1.0, 2.0)
    layers = 2.0 ** jax.random.uniform(kl, (LAYERS, 1, 1), jnp.float32, -1.0, 1.0)
    times = {"wq": 1.0, "wk": 1.0, "wv": 2.0, "wo": layers, "w_gate": 1.0, "w_up": bump(kh, FF, 4.0), "w_down": layers}
    x = together(ka, jax.random.normal(kx, shape, jnp.float32), much_x) * bump(kf, D, 4.0)
    dy = together(kb, jax.random.normal(kdy, shape, jnp.float32), much_dy)
    drawn = {"x": x.astype(jnp.bfloat16), "dy": (loud * dy * (SEQUENCES * TOKENS) ** -0.5).astype(jnp.bfloat16)}
    for key, name in zip(kw, NAMES, strict=True):
        drawn[name] = (jax.random.normal(key, SHAPES[name], jnp.float32) * SHAPES[name][1] ** -0.5 * times[name]).astype(jnp.bfloat16)
    for key, name in zip(km, NAMES, strict=True):
        drawn[f"m_{name}"] = 0.1 * jax.random.normal(key, SHAPES[name], jnp.float32)
    for key, name in zip(kv, NAMES, strict=True):
        drawn[f"v_{name}"] = loud * loud * jax.random.uniform(key, SHAPES[name], jnp.float32, 0.2, 0.6)
    return drawn


def matmul(a, w):
    return jnp.dot(a, w, preferred_element_type=jnp.float32).astype(jnp.bfloat16)


def normed(h):
    wide = h.astype(jnp.float32)
    scale = lax.rsqrt(jnp.mean(wide**2, -1, keepdims=True) + 1e-6)
    return (wide * scale).astype(jnp.bfloat16)


def turned(t, theta):
    half = t.shape[-1] // 2
    angle = jnp.arange(t.shape[0], dtype=jnp.float32)[:, None] * theta ** (-jnp.arange(half, dtype=jnp.float32) / half)
    cos, sin = jnp.cos(angle)[:, None], jnp.sin(angle)[:, None]
    a, b = t[..., :half].astype(jnp.float32), t[..., half:].astype(jnp.float32)
    return jnp.concatenate([a * cos - b * sin, b * cos + a * sin], -1).astype(jnp.bfloat16)


def seen_by(q, k, v):
    tokens, kv = q.shape[0], k.shape[1]
    q = q.reshape(tokens, kv, -1, q.shape[-1])
    scores = jnp.einsum("tgsd,ugd->gstu", q.astype(jnp.float32), k.astype(jnp.float32)) * q.shape[-1] ** -0.5
    place = jnp.arange(tokens)
    weights = jax.nn.softmax(jnp.where(place[:, None] >= place, scores, -jnp.inf), -1).astype(jnp.bfloat16)
    return jnp.einsum("gstu,ugd->tgsd", weights.astype(jnp.float32), v.astype(jnp.float32)).astype(jnp.bfloat16).reshape(tokens, -1)


def layer(h, w):
    a = normed(h)
    q, k = (turned(matmul(a, w[name]).reshape(h.shape[0], -1, HEAD), THETA) for name in ("wq", "wk"))
    h = h + matmul(seen_by(q, k, matmul(a, w["wv"]).reshape(h.shape[0], -1, HEAD)), w["wo"])
    b = normed(h)
    gate = jnp.dot(b, w["w_gate"], preferred_element_type=jnp.float32)
    up = jnp.dot(b, w["w_up"], preferred_element_type=jnp.float32)
    return h + matmul((jax.nn.silu(gate) * up).astype(jnp.bfloat16), w["w_down"])


def adamw(w, m, v, g):
    m = 0.9 * m + 0.1 * g
    v = 0.95 * v + 0.05 * g * g
    step = m * lax.rsqrt(v + 1e-8) + 0.1 * w
    return (w - 0.02 * step).astype(jnp.bfloat16), m, v


def stack(weights, h):
    return lax.scan(lambda h, w: (layer(h, w), None), h, weights)[0]


def reference(x, dy, wq, wk, wv, wo, w_gate, w_up, w_down, m_wq, m_wk, m_wv, m_wo, m_w_gate, m_w_up, m_w_down, v_wq, v_wk, v_wv, v_wo, v_w_gate, v_w_up, v_w_down):
    weights = dict(zip(NAMES, (wq, wk, wv, wo, w_gate, w_up, w_down), strict=True))

    def take(so_far, sequence):
        h, by_y = sequence
        _, back = jax.vjp(stack, weights, h)
        by_weights, by_h = back(by_y)
        return jax.tree.map(lambda total, term: total + term.astype(jnp.float32), so_far, by_weights), by_h

    none_yet = {name: jnp.zeros(w.shape, jnp.float32) for name, w in weights.items()}
    by_weights, by_x = lax.scan(take, none_yet, (x, dy))
    gradients = [by_weights[name].astype(jnp.bfloat16).astype(jnp.float32) for name in NAMES]
    first = (m_wq, m_wk, m_wv, m_wo, m_w_gate, m_w_up, m_w_down)
    second = (v_wq, v_wk, v_wv, v_wo, v_w_gate, v_w_up, v_w_down)
    new = [adamw(weights[name].astype(jnp.float32), m, v, g) for name, m, v, g in zip(NAMES, first, second, gradients, strict=True)]
    return tuple(one[which] for which in range(3) for one in new)
```

```python
import functools

import jax
import jax.numpy as jnp
from jax import lax
from jax.experimental import pallas as pl
from jax.experimental.pallas import tpu as pltpu
from jax.sharding import PartitionSpec as P

NEG = -1e30
HIDDEN = 2 * NEG
LOG2E = 1.4426950408889634
VMEM = 60 * 2**20
HEAD = 128
HALF = HEAD // 2
THETA = 10000
NAMES = ("wq", "wk", "wv", "wo", "w_gate", "w_up", "w_down")
F32, BF16 = jnp.float32, jnp.bfloat16

FQ, FK, FH = 512, 512, 1
BQ, BK, BH = 256, 256, 1
ROWS = 512
CHUNK = 512


def _dot(a, b, ca, cb):
    return lax.dot_general(a, b, (((ca,), (cb,)), ((), ())), preferred_element_type=F32)


def _params(*semantics):
    return pltpu.CompilerParams(dimension_semantics=semantics, vmem_limit_bytes=VMEM)


def _cost(flops, arrays, exps=0):
    return pl.CostEstimate(flops=int(flops), transcendentals=int(exps), bytes_accessed=int(sum(a.size * a.dtype.itemsize for a in arrays)))


def _sds(shape, dtype=BF16):
    return jax.ShapeDtypeStruct(shape, dtype)


def _rows(width, rows=None):
    return pl.BlockSpec((rows or ROWS, width), lambda i: (i, 0))


def _whole(shape, at=(0, 0)):
    return pl.BlockSpec(shape, lambda i: at, pipeline_mode=pl.Buffered(1))


def _strips(heads, per):
    return [tuple(range(h, h + per)) for h in range(0, heads, per)]


def _strip(ref, strip):
    return jnp.concatenate([ref[:, h * HEAD : (h + 1) * HEAD] for h in strip], axis=0)


def _gap(bk, bq, per):
    row = lax.broadcasted_iota(jnp.int32, (bk, bq), 1) - lax.broadcasted_iota(jnp.int32, (bk, bq), 0)
    return jnp.concatenate([row] * per, axis=1)


def _spans(iq, bq, bk):
    return lax.div(iq * bq + 1, bk), lax.div(iq * bq + bq + bk - 1, bk)


def _attend_kernel(q_ref, k_ref, v_ref, o_ref, lse_ref, top_s, mix_s, gap_s, *, bq, bk, per):
    heads = q_ref.shape[1] // HEAD
    strips = _strips(heads, per)
    iq = pl.program_id(0)
    e = HEAD**-0.5 * LOG2E

    @pl.when(iq == 0)
    def _():
        gap_s[...] = _gap(bk, bq, per)

    top_s[...] = jnp.full_like(top_s, NEG)
    mix_s[...] = jnp.zeros_like(mix_s)
    ones = jnp.ones((8, bk), BF16)

    def block(j, masked):
        here = pl.ds(pl.multiple_of(j * bk, bk), bk)
        keys = k_ref[here, :]
        scores = [_dot(keys, _strip(q_ref, s), 1, 1) for s in strips]
        ok = gap_s[...] >= j * bk - iq * bq if masked else None
        weights, keeps = [], []
        for n, s in enumerate(scores):
            if masked:
                s = jnp.where(ok, s, HIDDEN)
            old = top_s[n : n + 1, :]
            top = jnp.maximum(old, s.max(axis=0, keepdims=True))
            top_s[n : n + 1, :] = top
            weights.append(jnp.exp2((s - top) * e).astype(BF16))
            keeps.append(jnp.exp2((old - top) * e))
        values = jnp.concatenate([v_ref[here, :].T, ones], axis=0)
        for n, (p, keep) in enumerate(zip(weights, keeps)):
            mix_s[n] = mix_s[n] * keep + _dot(values, p, 1, 0)

    whole, last = _spans(iq, bq, bk)
    lax.fori_loop(0, whole, lambda j, _: block(j, False), None)
    lax.fori_loop(whole, last, lambda j, _: block(j, True), None)
    for n, strip in enumerate(strips):
        total = mix_s[n, HEAD : HEAD + 1, :]
        out = (mix_s[n, :HEAD, :] * (1 / total)).T.astype(BF16)
        lse = top_s[n : n + 1, :] * e + jnp.log2(total)
        for i, h in enumerate(strip):
            o_ref[:, h * HEAD : (h + 1) * HEAD] = out[i * bq : (i + 1) * bq, :]
            lse_ref[h : h + 1, :] = lse[:, i * bq : (i + 1) * bq]


def attend(q, k, v, bq=None, bk=None, per=None):
    bq, bk, per = bq or FQ, bk or FK, per or FH
    tokens, width = q.shape
    heads = width // HEAD
    strips = heads // per
    keys = pl.BlockSpec((tokens, HEAD), lambda i: (0, 0))
    return pl.pallas_call(
        functools.partial(_attend_kernel, bq=bq, bk=bk, per=per),
        grid=(tokens // bq,),
        in_specs=[_rows(width, bq), keys, keys],
        out_specs=[_rows(width, bq), pl.BlockSpec((heads, bq), lambda i: (0, i))],
        out_shape=[_sds(q.shape), _sds((heads, tokens), F32)],
        scratch_shapes=[pltpu.VMEM((strips, per * bq), F32), pltpu.VMEM((strips, HEAD + 8, per * bq), F32), pltpu.VMEM((bk, per * bq), jnp.int32)],
        compiler_params=_params("arbitrary"),
        cost_estimate=_cost(4 * heads * tokens * tokens * HEAD, [q, q, k, v], heads * tokens * tokens),
        name="attend",
    )(q, k, v)


def _attend_bwd_kernel(q_ref, k_ref, v_ref, do_ref, o_ref, lse_ref, dq_ref, dk_ref, dv_ref, dq_s, dk_s, dv_s, gap_s, *, bq, bk, per):
    heads = q_ref.shape[1] // HEAD
    strips = _strips(heads, per)
    iq = pl.program_id(0)
    scale = HEAD**-0.5
    e = scale * LOG2E

    @pl.when(iq == 0)
    def _():
        gap_s[...] = _gap(bk, bq, per)
        dk_s[...] = jnp.zeros_like(dk_s)
        dv_s[...] = jnp.zeros_like(dv_s)

    dq_s[...] = jnp.zeros_like(dq_s)
    lses, deltas = [], []
    for strip in strips:
        lses.append(jnp.concatenate([lse_ref[h : h + 1, :] for h in strip], axis=1))
        both = _strip(do_ref, strip).astype(F32) * _strip(o_ref, strip).astype(F32)
        deltas.append(both.T.sum(axis=0, keepdims=True))

    def block(j, masked):
        here = pl.ds(pl.multiple_of(j * bk, bk), bk)
        keys, values = k_ref[here, :], v_ref[here, :]
        qs, dos = [_strip(q_ref, s) for s in strips], [_strip(do_ref, s) for s in strips]
        scores = [_dot(keys, x, 1, 1) for x in qs]
        dps = [_dot(values, x, 1, 1) for x in dos]
        ok = gap_s[...] >= j * bk - iq * bq if masked else None
        flat = keys.T
        for n in range(len(strips)):
            p = jnp.exp2(scores[n] * e - lses[n])
            if masked:
                p = jnp.where(ok, p, 0.0)
            ds = (p * (dps[n] - deltas[n])).astype(BF16)
            dv_s[here, :] += _dot(p.astype(BF16), dos[n], 1, 0)
            dk_s[here, :] += _dot(ds, qs[n], 1, 0)
            dq_s[n] += _dot(flat, ds, 1, 0)

    whole, last = _spans(iq, bq, bk)
    lax.fori_loop(0, whole, lambda j, _: block(j, False), None)
    lax.fori_loop(whole, last, lambda j, _: block(j, True), None)
    for n, strip in enumerate(strips):
        dq = (dq_s[n] * scale).T.astype(BF16)
        for i, h in enumerate(strip):
            dq_ref[:, h * HEAD : (h + 1) * HEAD] = dq[i * bq : (i + 1) * bq, :]

    @pl.when(iq == pl.num_programs(0) - 1)
    def _():
        dk_ref[...] = (dk_s[...] * scale).astype(BF16)
        dv_ref[...] = dv_s[...].astype(BF16)


def attend_bwd(q, k, v, d_out, out, lse, bq=None, bk=None, per=None):
    bq, bk, per = bq or BQ, bk or BK, per or BH
    tokens, width = q.shape
    heads = width // HEAD
    strips = heads // per
    keys = pl.BlockSpec((tokens, HEAD), lambda i: (0, 0))
    rows = _rows(width, bq)
    return pl.pallas_call(
        functools.partial(_attend_bwd_kernel, bq=bq, bk=bk, per=per),
        grid=(tokens // bq,),
        in_specs=[rows, keys, keys, rows, rows, pl.BlockSpec((heads, bq), lambda i: (0, i))],
        out_specs=[rows, keys, keys],
        out_shape=[_sds(q.shape), _sds(k.shape), _sds(v.shape)],
        scratch_shapes=[pltpu.VMEM((strips, HEAD, per * bq), F32), pltpu.VMEM((tokens, HEAD), F32), pltpu.VMEM((tokens, HEAD), F32),
                        pltpu.VMEM((bk, per * bq), jnp.int32)],
        compiler_params=_params("arbitrary"),
        cost_estimate=_cost(10 * heads * tokens * tokens * HEAD, [q, q, q, q, k, k, v, v], heads * tokens * tokens),
        name="attend_bwd",
    )(q, k, v, d_out, out, lse)


def _normed(h):
    scale = lax.rsqrt(jnp.mean(h * h, -1, keepdims=True) + 1e-6)
    return (h * scale).astype(BF16), scale


def _normed_bwd(h, scale, by):
    return scale * by - h * (scale * scale * scale * jnp.mean(by * h, -1, keepdims=True))


def _turn(t, cos, sin):
    t = t.astype(F32)
    return (t * cos + pltpu.roll(t, HALF, 1) * sin).astype(BF16)


def _qkv_kernel(h_ref, w_ref, cos_ref, sin_ref, q_ref, k_ref, v_ref):
    a, _ = _normed(h_ref[...].astype(F32))
    cos, sin = cos_ref[...], sin_ref[...]
    wide = q_ref.shape[1]
    for at in range(0, wide, 2 * HEAD):
        t = _dot(a, w_ref[:, at : at + 2 * HEAD], 1, 0).astype(BF16)
        q_ref[:, at : at + HEAD] = _turn(t[:, :HEAD], cos, sin)
        q_ref[:, at + HEAD : at + 2 * HEAD] = _turn(t[:, HEAD:], cos, sin)
    t = _dot(a, w_ref[:, wide:], 1, 0).astype(BF16)
    k_ref[...] = _turn(t[:, :HEAD], cos, sin)
    v_ref[...] = t[:, HEAD:]


def qkv(h, w, cos, sin):
    tokens, d = h.shape
    wide = w.shape[1] - 2 * HEAD
    return pl.pallas_call(
        _qkv_kernel,
        grid=(tokens // ROWS,),
        in_specs=[_rows(d), _whole(w.shape), _rows(HEAD), _rows(HEAD)],
        out_specs=[_rows(wide), _rows(HEAD), _rows(HEAD)],
        out_shape=[_sds((tokens, wide)), _sds((tokens, HEAD)), _sds((tokens, HEAD))],
        compiler_params=_params("arbitrary"),
        cost_estimate=_cost(2 * tokens * w.size, [h, w, cos, sin]),
        name="qkv",
    )(h, w, cos, sin)


def _qkv_bwd_kernel(h_ref, w_ref, cos_ref, sin_ref, dq_ref, dk_ref, dv_ref, *rest, onward):
    by_ref, out_ref, dw_ref, total, turned = rest if onward else (None, None, *rest)
    h = h_ref[...].astype(F32)
    a, scale = _normed(h)
    cos, sin = cos_ref[...], -sin_ref[...]
    wide = dq_ref.shape[1]
    for at in range(0, wide, HEAD):
        turned[:, at : at + HEAD] = _turn(dq_ref[:, at : at + HEAD], cos, sin)
    turned[:, wide : wide + HEAD] = _turn(dk_ref[...], cos, sin)
    turned[:, wide + HEAD :] = dv_ref[...]

    @pl.when(pl.program_id(0) == 0)
    def _():
        total[...] = jnp.zeros_like(total)

    total[...] += _dot(a, turned[...], 0, 0)
    if onward:
        by_a = _dot(turned[...], w_ref[...], 1, 1)
        out_ref[...] = (by_ref[...].astype(F32) + _normed_bwd(h, scale, by_a)).astype(BF16)

    @pl.when(pl.program_id(0) == pl.num_programs(0) - 1)
    def _():
        dw_ref[...] = total[...].astype(BF16)


def qkv_bwd(h, w, cos, sin, dq, dk, dv, by=None):
    tokens, d = h.shape
    onward = by is not None
    got = pl.pallas_call(
        functools.partial(_qkv_bwd_kernel, onward=onward),
        grid=(tokens // ROWS,),
        in_specs=[_rows(d), _whole(w.shape), _rows(HEAD), _rows(HEAD), _rows(dq.shape[1]), _rows(HEAD), _rows(HEAD)] + [_rows(d)] * onward,
        out_specs=[_rows(d)] * onward + [_whole(w.shape)],
        out_shape=[_sds(h.shape)] * onward + [_sds(w.shape)],
        scratch_shapes=[pltpu.VMEM(w.shape, F32), pltpu.VMEM((ROWS, w.shape[1]), BF16)],
        compiler_params=_params("arbitrary"),
        cost_estimate=_cost((2 + 2 * onward) * tokens * w.size, [h, w, cos, sin, dq, dk, dv]),
        name="qkv_bwd",
    )(h, w, cos, sin, dq, dk, dv, *([by] if onward else []))
    return got if onward else (None, got[0])


def _post_kernel(h_ref, o_ref, wo_ref, gate_ref, up_ref, down_ref, mid_ref, out_ref):
    mid = (h_ref[...].astype(F32) + _dot(o_ref[...], wo_ref[...], 1, 0).astype(BF16).astype(F32)).astype(BF16)
    mid_ref[...] = mid
    b, _ = _normed(mid.astype(F32))
    total = None
    for at in range(0, gate_ref.shape[1], CHUNK):
        gate = _dot(b, gate_ref[:, at : at + CHUNK], 1, 0)
        up = _dot(b, up_ref[:, at : at + CHUNK], 1, 0)
        term = _dot((gate * jax.nn.sigmoid(gate) * up).astype(BF16), down_ref[at : at + CHUNK, :], 1, 0)
        total = term if total is None else total + term
    out_ref[...] = (mid.astype(F32) + total.astype(BF16).astype(F32)).astype(BF16)


def post(h, o, w_od, w_gu):
    tokens, d = h.shape
    ff, wide = w_gu.shape[1] // 2, o.shape[1]
    return pl.pallas_call(
        _post_kernel,
        grid=(tokens // ROWS,),
        in_specs=[_rows(d), _rows(wide), _whole((wide, d)), _whole((d, ff)), _whole((d, ff), (0, 1)), _whole((ff, d), (0, 1))],
        out_specs=[_rows(d), _rows(d)],
        out_shape=[_sds(h.shape), _sds(h.shape)],
        compiler_params=_params("arbitrary"),
        cost_estimate=_cost(2 * tokens * (w_od.size + w_gu.size), [h, h, h, o, w_od, w_gu], tokens * ff),
        name="post",
    )(h, o, w_od, w_gu, w_gu, w_od)


def _post_bwd_kernel(h_ref, o_ref, by_ref, wo_ref, gate_ref, up_ref, down_ref, out_ref, do_ref, d_od_ref, d_gu_ref, od_s, gu_s, *, again):
    ff, d = down_ref.shape
    by = by_ref[...]
    mid = h_ref[...]
    if again:
        mid = (mid.astype(F32) + _dot(o_ref[...], wo_ref[...], 1, 0).astype(BF16).astype(F32)).astype(BF16)
    mid = mid.astype(F32)
    b, scale = _normed(mid)

    @pl.when(pl.program_id(0) == 0)
    def _():
        od_s[...] = jnp.zeros_like(od_s)
        gu_s[...] = jnp.zeros_like(gu_s)

    by_b = None
    for at in range(0, ff, CHUNK):
        here = slice(at, at + CHUNK)
        gate = _dot(b, gate_ref[:, here], 1, 0)
        up = _dot(b, up_ref[:, here], 1, 0)
        by_act = _dot(by, down_ref[here, :], 1, 1).astype(BF16).astype(F32)
        part = jax.nn.sigmoid(gate)
        silu = gate * part
        by_up = (by_act * silu).astype(BF16)
        by_gate = (by_act * up * (part + silu * (1 - part))).astype(BF16)
        od_s[here, d:] += _dot((silu * up).astype(BF16), by, 0, 0)
        gu_s[:, here] += _dot(b, by_gate, 0, 0)
        gu_s[:, ff + at : ff + at + CHUNK] += _dot(b, by_up, 0, 0)
        term = _dot(by_gate, gate_ref[:, here], 1, 1) + _dot(by_up, up_ref[:, here], 1, 1)
        by_b = term if by_b is None else by_b + term
    by_mid = (by.astype(F32) + _normed_bwd(mid, scale, by_b)).astype(BF16)
    out_ref[...] = by_mid
    do_ref[...] = _dot(by_mid, wo_ref[...], 1, 1).astype(BF16)
    od_s[:, :d] += _dot(o_ref[...], by_mid, 0, 0)

    @pl.when(pl.program_id(0) == pl.num_programs(0) - 1)
    def _():
        d_od_ref[...] = od_s[...].astype(BF16)
        d_gu_ref[...] = gu_s[...].astype(BF16)


def post_bwd(h, o, by, w_od, w_gu, again):
    tokens, d = h.shape
    ff, wide = w_gu.shape[1] // 2, o.shape[1]
    return pl.pallas_call(
        functools.partial(_post_bwd_kernel, again=again),
        grid=(tokens // ROWS,),
        in_specs=[_rows(d), _rows(wide), _rows(d), _whole((wide, d)), _whole((d, ff)), _whole((d, ff), (0, 1)), _whole((ff, d), (0, 1))],
        out_specs=[_rows(d), _rows(wide), _whole(w_od.shape), _whole(w_gu.shape)],
        out_shape=[_sds(h.shape), _sds(o.shape), _sds(w_od.shape), _sds(w_gu.shape)],
        scratch_shapes=[pltpu.VMEM(w_od.shape, F32), pltpu.VMEM(w_gu.shape, F32)],
        compiler_params=_params("arbitrary"),
        cost_estimate=_cost(4 * tokens * (w_od.size + w_gu.size) + 2 * tokens * w_gu.size, [h, h, h, o, o, w_od, w_gu, w_od, w_gu], tokens * ff),
        name="post_bwd",
    )(h, o, by, w_od, w_gu, w_gu, w_od)


def adamw(w, m, v, g):
    m = 0.9 * m + 0.1 * g
    v = 0.95 * v + 0.05 * g * g
    step = m * lax.rsqrt(v + 1e-8) + 0.1 * w
    return (w - 0.02 * step).astype(BF16), m, v


def tables(tokens):
    angle = jnp.arange(tokens, dtype=F32)[:, None] * THETA ** (-jnp.arange(HALF, dtype=F32) / HALF)
    cos, sin = jnp.cos(angle), jnp.sin(angle)
    return jnp.concatenate([cos, cos], -1), jnp.concatenate([-sin, sin], -1)


def solution(mesh):
    def gathered(*blocks):
        return lax.all_gather(jnp.concatenate(blocks, axis=1), "dp", axis=0, tiled=True)

    def scattered(gradient):
        return lax.psum_scatter(gradient, "dp", scatter_dimension=0, tiled=True)

    def after_that(value, sums):
        return lax.optimization_barrier((value, sums))

    def step(x, dy, *arrays):
        weights, m, v = (arrays[i : i + 7] for i in (0, 7, 14))
        layers = weights[0].shape[0]
        x, by = x[0], dy[0]
        whole = []
        for n in range(layers):
            wq, wk, wv, wo, gate, up, down = (w[n] for w in weights)
            whole.append((gathered(wq, wk, wv), gathered(wo, down), gathered(gate, up)))
        cos, sin = tables(x.shape[0])
        h, kept = x, []
        for n, (w_qkv, w_od, w_gu) in enumerate(whole):
            q, k, v_ = qkv(h, w_qkv, cos, sin)
            o, lse = attend(q, k, v_)
            if n < layers - 1:
                mid, after = post(h, o, w_od, w_gu)
            else:
                mid, after = h, None
            kept.append((h, q, k, v_, o, lse, mid))
            h = after
        mine, above = [None] * layers, None
        for n in reversed(range(layers)):
            w_qkv, w_od, w_gu = whole[n]
            h, q, k, v_, o, lse, mid = kept[n]
            by_mid, by_o, d_od, d_gu = post_bwd(mid, o, by, w_od, w_gu, n == layers - 1)
            if n < layers - 1:
                by_o, above = after_that(by_o, above)
                mine[n + 1] = (above, *mine[n + 1][1:])
            d_od, d_gu = scattered(d_od), scattered(d_gu)
            dq, dk, dv = attend_bwd(q, k, v_, by_o, o, lse)
            dq, d_od = after_that(dq, d_od)
            by, d_qkv = qkv_bwd(h, w_qkv, cos, sin, dq, dk, dv, by_mid if n else None)
            if n:
                by, d_gu = after_that(by, d_gu)
            else:
                d_qkv, d_gu = after_that(d_qkv, d_gu)
            above = scattered(d_qkv)
            mine[n] = above, d_od, d_gu
        d, ff, wide = x.shape[1], weights[4].shape[2], weights[0].shape[2]
        parts = []
        for d_qkv, d_od, d_gu in mine:
            parts.append((d_qkv[:, :wide], d_qkv[:, wide : wide + HEAD], d_qkv[:, wide + HEAD :], d_od[:, :d], d_gu[:, :ff], d_gu[:, ff:], d_od[:, d:]))
        new = []
        for i, (w, first, second) in enumerate(zip(weights, m, v, strict=True)):
            g = jnp.stack([part[i] for part in parts]).astype(F32)
            new.append(adamw(w.astype(F32), first, second, g))
        return tuple(one[which] for which in range(3) for one in new)

    states, cut = P(("rep", "dp"), None, None), P(None, "dp", None)
    return jax.shard_map(
        step,
        mesh=mesh,
        in_specs=(states, states) + (cut,) * 21,
        out_specs=(P("rep", "dp", None),) * 21,
        check_vma=False,
    )
```

```python
import functools

import jax
import jax.numpy as jnp
from jax import lax
from jax.experimental import pallas as pl
from jax.experimental.pallas import tpu as pltpu
from jax.sharding import PartitionSpec as P

NEG = -1e30
HIDDEN = 2 * NEG
LOG2E = 1.4426950408889634
VMEM = 60 * 2**20
HEAD = 128
HALF = HEAD // 2
THETA = 10000
NAMES = ("wq", "wk", "wv", "wo", "w_gate", "w_up", "w_down")
F32, BF16 = jnp.float32, jnp.bfloat16

FQ, FK, FH = 512, 512, 1
BQ, BK, BH = 256, 256, 1
ROWS = 512
FEW = 256
CHUNK = 768


def _dot(a, b, ca, cb):
    return lax.dot_general(a, b, (((ca,), (cb,)), ((), ())), preferred_element_type=F32)


def _params(*semantics):
    return pltpu.CompilerParams(dimension_semantics=semantics, vmem_limit_bytes=VMEM)


def _cost(flops, arrays, exps=0):
    return pl.CostEstimate(flops=int(flops), transcendentals=int(exps), bytes_accessed=int(sum(a.size * a.dtype.itemsize for a in arrays)))


def _sds(shape, dtype=BF16):
    return jax.ShapeDtypeStruct(shape, dtype)


def _rows(width, rows=None):
    return pl.BlockSpec((rows or ROWS, width), lambda i: (i, 0))


def _whole(shape, at=(0, 0)):
    return pl.BlockSpec(shape, lambda i: at, pipeline_mode=pl.Buffered(1))


def _strips(heads, per):
    return [tuple(range(h, h + per)) for h in range(0, heads, per)]


def _strip(ref, strip):
    return jnp.concatenate([ref[:, h * HEAD : (h + 1) * HEAD] for h in strip], axis=0)


def _gap(bk, bq, per):
    row = lax.broadcasted_iota(jnp.int32, (bk, bq), 1) - lax.broadcasted_iota(jnp.int32, (bk, bq), 0)
    return jnp.concatenate([row] * per, axis=1)


def _spans(iq, bq, bk):
    return lax.div(iq * bq + 1, bk), lax.div(iq * bq + bq + bk - 1, bk)


def _attend_kernel(q_ref, k_ref, v_ref, o_ref, lse_ref, top_s, mix_s, gap_s, *, bq, bk, per):
    heads = q_ref.shape[1] // HEAD
    strips = _strips(heads, per)
    iq = pl.program_id(0)
    e = HEAD**-0.5 * LOG2E

    @pl.when(iq == 0)
    def _():
        gap_s[...] = _gap(bk, bq, per)

    top_s[...] = jnp.full_like(top_s, NEG)
    mix_s[...] = jnp.zeros_like(mix_s)
    ones = jnp.ones((8, bk), BF16)

    def block(j, masked):
        here = pl.ds(pl.multiple_of(j * bk, bk), bk)
        keys = k_ref[here, :]
        scores = [_dot(keys, _strip(q_ref, s), 1, 1) for s in strips]
        ok = gap_s[...] >= j * bk - iq * bq if masked else None
        weights, keeps = [], []
        for n, s in enumerate(scores):
            if masked:
                s = jnp.where(ok, s, HIDDEN)
            old = top_s[n : n + 1, :]
            top = jnp.maximum(old, s.max(axis=0, keepdims=True))
            top_s[n : n + 1, :] = top
            weights.append(jnp.exp2((s - top) * e).astype(BF16))
            keeps.append(jnp.exp2((old - top) * e))
        values = jnp.concatenate([v_ref[here, :].T, ones], axis=0)
        for n, (p, keep) in enumerate(zip(weights, keeps)):
            mix_s[n] = mix_s[n] * keep + _dot(values, p, 1, 0)

    whole, last = _spans(iq, bq, bk)
    lax.fori_loop(0, whole, lambda j, _: block(j, False), None)
    lax.fori_loop(whole, last, lambda j, _: block(j, True), None)
    for n, strip in enumerate(strips):
        total = mix_s[n, HEAD : HEAD + 1, :]
        out = (mix_s[n, :HEAD, :] * (1 / total)).T.astype(BF16)
        lse = top_s[n : n + 1, :] * e + jnp.log2(total)
        for i, h in enumerate(strip):
            o_ref[:, h * HEAD : (h + 1) * HEAD] = out[i * bq : (i + 1) * bq, :]
            lse_ref[h : h + 1, :] = lse[:, i * bq : (i + 1) * bq]


def attend(q, k, v, bq=None, bk=None, per=None):
    bq, bk, per = bq or FQ, bk or FK, per or FH
    tokens, width = q.shape
    heads = width // HEAD
    strips = heads // per
    keys = pl.BlockSpec((tokens, HEAD), lambda i: (0, 0))
    return pl.pallas_call(
        functools.partial(_attend_kernel, bq=bq, bk=bk, per=per),
        grid=(tokens // bq,),
        in_specs=[_rows(width, bq), keys, keys],
        out_specs=[_rows(width, bq), pl.BlockSpec((heads, bq), lambda i: (0, i))],
        out_shape=[_sds(q.shape), _sds((heads, tokens), F32)],
        scratch_shapes=[pltpu.VMEM((strips, per * bq), F32), pltpu.VMEM((strips, HEAD + 8, per * bq), F32), pltpu.VMEM((bk, per * bq), jnp.int32)],
        compiler_params=_params("arbitrary"),
        cost_estimate=_cost(4 * heads * tokens * tokens * HEAD, [q, q, k, v], heads * tokens * tokens),
        name="attend",
    )(q, k, v)


def _attend_bwd_kernel(q_ref, k_ref, v_ref, do_ref, o_ref, lse_ref, dq_ref, dk_ref, dv_ref, dq_s, dk_s, dv_s, gap_s, *, bq, bk, per):
    heads = q_ref.shape[1] // HEAD
    strips = _strips(heads, per)
    iq = pl.program_id(0)
    scale = HEAD**-0.5
    e = scale * LOG2E

    @pl.when(iq == 0)
    def _():
        gap_s[...] = _gap(bk, bq, per)
        dk_s[...] = jnp.zeros_like(dk_s)
        dv_s[...] = jnp.zeros_like(dv_s)

    dq_s[...] = jnp.zeros_like(dq_s)
    lses, deltas = [], []
    for strip in strips:
        lses.append(jnp.concatenate([lse_ref[h : h + 1, :] for h in strip], axis=1))
        both = _strip(do_ref, strip).astype(F32) * _strip(o_ref, strip).astype(F32)
        deltas.append(both.T.sum(axis=0, keepdims=True))

    def block(j, masked):
        here = pl.ds(pl.multiple_of(j * bk, bk), bk)
        keys, values = k_ref[here, :], v_ref[here, :]
        qs, dos = [_strip(q_ref, s) for s in strips], [_strip(do_ref, s) for s in strips]
        scores = [_dot(keys, x, 1, 1) for x in qs]
        dps = [_dot(values, x, 1, 1) for x in dos]
        ok = gap_s[...] >= j * bk - iq * bq if masked else None
        flat = keys.T
        for n in range(len(strips)):
            p = jnp.exp2(scores[n] * e - lses[n])
            if masked:
                p = jnp.where(ok, p, 0.0)
            ds = (p * (dps[n] - deltas[n])).astype(BF16)
            dv_s[here, :] += _dot(p.astype(BF16), dos[n], 1, 0)
            dk_s[here, :] += _dot(ds, qs[n], 1, 0)
            dq_s[n] += _dot(flat, ds, 1, 0)

    whole, last = _spans(iq, bq, bk)
    lax.fori_loop(0, whole, lambda j, _: block(j, False), None)
    lax.fori_loop(whole, last, lambda j, _: block(j, True), None)
    for n, strip in enumerate(strips):
        dq = (dq_s[n] * scale).T.astype(BF16)
        for i, h in enumerate(strip):
            dq_ref[:, h * HEAD : (h + 1) * HEAD] = dq[i * bq : (i + 1) * bq, :]

    @pl.when(iq == pl.num_programs(0) - 1)
    def _():
        dk_ref[...] = (dk_s[...] * scale).astype(BF16)
        dv_ref[...] = dv_s[...].astype(BF16)


def attend_bwd(q, k, v, d_out, out, lse, bq=None, bk=None, per=None):
    bq, bk, per = bq or BQ, bk or BK, per or BH
    tokens, width = q.shape
    heads = width // HEAD
    strips = heads // per
    keys = pl.BlockSpec((tokens, HEAD), lambda i: (0, 0))
    rows = _rows(width, bq)
    return pl.pallas_call(
        functools.partial(_attend_bwd_kernel, bq=bq, bk=bk, per=per),
        grid=(tokens // bq,),
        in_specs=[rows, keys, keys, rows, rows, pl.BlockSpec((heads, bq), lambda i: (0, i))],
        out_specs=[rows, keys, keys],
        out_shape=[_sds(q.shape), _sds(k.shape), _sds(v.shape)],
        scratch_shapes=[pltpu.VMEM((strips, HEAD, per * bq), F32), pltpu.VMEM((tokens, HEAD), F32), pltpu.VMEM((tokens, HEAD), F32),
                        pltpu.VMEM((bk, per * bq), jnp.int32)],
        compiler_params=_params("arbitrary"),
        cost_estimate=_cost(10 * heads * tokens * tokens * HEAD, [q, q, q, q, k, k, v, v], heads * tokens * tokens),
        name="attend_bwd",
    )(q, k, v, d_out, out, lse)


def _normed(h):
    scale = lax.rsqrt(jnp.mean(h * h, -1, keepdims=True) + 1e-6)
    return (h * scale).astype(BF16), scale


def _normed_bwd(h, scale, by):
    return scale * by - h * (scale * scale * scale * jnp.mean(by * h, -1, keepdims=True))


def _turn(t, cos, sin):
    t = t.astype(F32)
    return (t * cos + pltpu.roll(t, HALF, 1) * sin).astype(BF16)


def _qkv_kernel(h_ref, w_ref, cos_ref, sin_ref, q_ref, k_ref, v_ref):
    a, _ = _normed(h_ref[...].astype(F32))
    cos, sin = cos_ref[...], sin_ref[...]
    wide = q_ref.shape[1]
    for at in range(0, wide, 2 * HEAD):
        t = _dot(a, w_ref[:, at : at + 2 * HEAD], 1, 0).astype(BF16)
        q_ref[:, at : at + HEAD] = _turn(t[:, :HEAD], cos, sin)
        q_ref[:, at + HEAD : at + 2 * HEAD] = _turn(t[:, HEAD:], cos, sin)
    t = _dot(a, w_ref[:, wide:], 1, 0).astype(BF16)
    k_ref[...] = _turn(t[:, :HEAD], cos, sin)
    v_ref[...] = t[:, HEAD:]


def qkv(h, w, cos, sin):
    tokens, d = h.shape
    wide = w.shape[1] - 2 * HEAD
    return pl.pallas_call(
        _qkv_kernel,
        grid=(tokens // ROWS,),
        in_specs=[_rows(d), _whole(w.shape), _rows(HEAD), _rows(HEAD)],
        out_specs=[_rows(wide), _rows(HEAD), _rows(HEAD)],
        out_shape=[_sds((tokens, wide)), _sds((tokens, HEAD)), _sds((tokens, HEAD))],
        compiler_params=_params("arbitrary"),
        cost_estimate=_cost(2 * tokens * w.size, [h, w, cos, sin]),
        name="qkv",
    )(h, w, cos, sin)


def _qkv_bwd_kernel(h_ref, w_ref, cos_ref, sin_ref, dq_ref, dk_ref, dv_ref, *rest, onward):
    by_ref, out_ref, dw_ref, total, turned = rest if onward else (None, None, *rest)
    h = h_ref[...].astype(F32)
    a, scale = _normed(h)
    cos, sin = cos_ref[...], -sin_ref[...]
    wide = dq_ref.shape[1]
    for at in range(0, wide, HEAD):
        turned[:, at : at + HEAD] = _turn(dq_ref[:, at : at + HEAD], cos, sin)
    turned[:, wide : wide + HEAD] = _turn(dk_ref[...], cos, sin)
    turned[:, wide + HEAD :] = dv_ref[...]

    @pl.when(pl.program_id(0) == 0)
    def _():
        total[...] = jnp.zeros_like(total)

    total[...] += _dot(a, turned[...], 0, 0)
    if onward:
        by_a = _dot(turned[...], w_ref[...], 1, 1)
        out_ref[...] = (by_ref[...].astype(F32) + _normed_bwd(h, scale, by_a)).astype(BF16)

    @pl.when(pl.program_id(0) == pl.num_programs(0) - 1)
    def _():
        dw_ref[...] = total[...].astype(BF16)


def qkv_bwd(h, w, cos, sin, dq, dk, dv, by=None):
    tokens, d = h.shape
    onward = by is not None
    got = pl.pallas_call(
        functools.partial(_qkv_bwd_kernel, onward=onward),
        grid=(tokens // ROWS,),
        in_specs=[_rows(d), _whole(w.shape), _rows(HEAD), _rows(HEAD), _rows(dq.shape[1]), _rows(HEAD), _rows(HEAD)] + [_rows(d)] * onward,
        out_specs=[_rows(d)] * onward + [_whole(w.shape)],
        out_shape=[_sds(h.shape)] * onward + [_sds(w.shape)],
        scratch_shapes=[pltpu.VMEM(w.shape, F32), pltpu.VMEM((ROWS, w.shape[1]), BF16)],
        compiler_params=_params("arbitrary"),
        cost_estimate=_cost((2 + 2 * onward) * tokens * w.size, [h, w, cos, sin, dq, dk, dv]),
        name="qkv_bwd",
    )(h, w, cos, sin, dq, dk, dv, *([by] if onward else []))
    return got if onward else (None, got[0])


def _post_kernel(h_ref, o_ref, wo_ref, gate_ref, up_ref, down_ref, mid_ref, out_ref):
    mid = (h_ref[...].astype(F32) + _dot(o_ref[...], wo_ref[...], 1, 0).astype(BF16).astype(F32)).astype(BF16)
    mid_ref[...] = mid
    b, _ = _normed(mid.astype(F32))
    total = None
    for at in range(0, gate_ref.shape[1], CHUNK):
        gate = _dot(b, gate_ref[:, at : at + CHUNK], 1, 0)
        up = _dot(b, up_ref[:, at : at + CHUNK], 1, 0)
        term = _dot((gate * jax.nn.sigmoid(gate) * up).astype(BF16), down_ref[at : at + CHUNK, :], 1, 0)
        total = term if total is None else total + term
    out_ref[...] = (mid.astype(F32) + total.astype(BF16).astype(F32)).astype(BF16)


def post(h, o, w_od, w_gu):
    tokens, d = h.shape
    ff, wide = w_od.shape[0], o.shape[1]
    return pl.pallas_call(
        _post_kernel,
        grid=(tokens // FEW,),
        in_specs=[_rows(d, FEW), _rows(wide, FEW), _whole((wide, d)), _whole((d, ff)), _whole((d, ff), (0, 1)), _whole((ff, d), (0, 1))],
        out_specs=[_rows(d, FEW), _rows(d, FEW)],
        out_shape=[_sds(h.shape), _sds(h.shape)],
        compiler_params=_params("arbitrary"),
        cost_estimate=_cost(2 * tokens * (w_od.size + w_gu.size), [h, h, h, o, w_od, w_gu], tokens * ff),
        name="post",
    )(h, o, w_od, w_gu, w_gu, w_od)


def _post_bwd_kernel(h_ref, o_ref, by_ref, wo_ref, gate_ref, up_ref, down_ref, out_ref, do_ref, d_od_ref, d_gu_ref, od_s, gu_s, *, again):
    ff, d = down_ref.shape
    by = by_ref[...]
    mid = h_ref[...]
    if again:
        mid = (mid.astype(F32) + _dot(o_ref[...], wo_ref[...], 1, 0).astype(BF16).astype(F32)).astype(BF16)
    mid = mid.astype(F32)
    b, scale = _normed(mid)

    @pl.when(pl.program_id(0) == 0)
    def _():
        od_s[...] = jnp.zeros_like(od_s)
        gu_s[...] = jnp.zeros_like(gu_s)

    b_flat, by_b = b.T, None
    for at in range(0, ff, CHUNK):
        here = slice(at, at + CHUNK)
        gate = _dot(b, gate_ref[:, here], 1, 0)
        up = _dot(b, up_ref[:, here], 1, 0)
        by_act = _dot(by, down_ref[here, :], 1, 1).astype(BF16).astype(F32)
        part = jax.nn.sigmoid(gate)
        silu = gate * part
        by_up = (by_act * silu).astype(BF16)
        by_gate = (by_act * up * (part + silu * (1 - part))).astype(BF16)
        od_s[here, d:] += _dot((silu * up).astype(BF16), by, 0, 0)
        both = _dot(b_flat, jnp.concatenate([by_gate, by_up], axis=1), 1, 0)
        gu_s[:, here] += both[:, :CHUNK]
        gu_s[:, ff + at : ff + at + CHUNK] += both[:, CHUNK:]
        term = _dot(by_gate, gate_ref[:, here], 1, 1) + _dot(by_up, up_ref[:, here], 1, 1)
        by_b = term if by_b is None else by_b + term
    by_mid = (by.astype(F32) + _normed_bwd(mid, scale, by_b)).astype(BF16)
    out_ref[...] = by_mid
    do_ref[...] = _dot(by_mid, wo_ref[...], 1, 1).astype(BF16)
    od_s[:, :d] += _dot(o_ref[...], by_mid, 0, 0)

    @pl.when(pl.program_id(0) == pl.num_programs(0) - 1)
    def _():
        d_od_ref[...] = od_s[...].astype(BF16)
        d_gu_ref[...] = gu_s[...].astype(BF16)


def post_bwd(h, o, by, w_od, w_gu, again):
    tokens, d = h.shape
    ff, wide = w_od.shape[0], o.shape[1]
    return pl.pallas_call(
        functools.partial(_post_bwd_kernel, again=again),
        grid=(tokens // FEW,),
        in_specs=[_rows(d, FEW), _rows(wide, FEW), _rows(d, FEW), _whole((wide, d)), _whole((d, ff)), _whole((d, ff), (0, 1)), _whole((ff, d), (0, 1))],
        out_specs=[_rows(d, FEW), _rows(wide, FEW), _whole(w_od.shape), _whole((d, 2 * ff))],
        out_shape=[_sds(h.shape), _sds(o.shape), _sds(w_od.shape), _sds((d, 2 * ff))],
        scratch_shapes=[pltpu.VMEM(w_od.shape, F32), pltpu.VMEM((d, 2 * ff), F32)],
        compiler_params=_params("arbitrary"),
        cost_estimate=_cost(4 * tokens * (w_od.size + w_gu.size) + 2 * tokens * w_gu.size, [h, h, h, o, o, w_od, w_gu, w_od, w_gu], tokens * ff),
        name="post_bwd",
    )(h, o, by, w_od, w_gu, w_gu, w_od)


def adamw(w, m, v, g):
    m = 0.9 * m + 0.1 * g
    v = 0.95 * v + 0.05 * g * g
    step = m * lax.rsqrt(v + 1e-8) + 0.1 * w
    return (w - 0.02 * step).astype(BF16), m, v


def tables(tokens):
    angle = jnp.arange(tokens, dtype=F32)[:, None] * THETA ** (-jnp.arange(HALF, dtype=F32) / HALF)
    cos, sin = jnp.cos(angle), jnp.sin(angle)
    return jnp.concatenate([cos, cos], -1), jnp.concatenate([-sin, sin], -1)


def solution(mesh):
    def gathered(*blocks):
        return lax.all_gather(jnp.concatenate(blocks, axis=1), "dp", axis=0, tiled=True)

    def scattered(gradient):
        return lax.psum_scatter(gradient, "dp", scatter_dimension=0, tiled=True)

    def after_that(value, sums):
        return lax.optimization_barrier((value, sums))

    def step(x, dy, *arrays):
        weights, m, v = (arrays[i : i + 7] for i in (0, 7, 14))
        layers = weights[0].shape[0]
        x, by = x[0], dy[0]
        whole, w_qkv = [], gathered(*(w[0] for w in weights[:3]))
        for n in range(layers):
            wo, gate, up, down = (w[n] for w in weights[3:])
            following = [w[n + 1] for w in weights[:3]] if n < layers - 1 else []
            w_od, w_gu = gathered(wo, down), gathered(gate, up, *following)
            whole.append((w_qkv, w_od, w_gu))
            w_qkv = w_gu[:, 2 * gate.shape[1] :]
        cos, sin = tables(x.shape[0])
        h, kept = x, []
        for n, (w_qkv, w_od, w_gu) in enumerate(whole):
            q, k, v_ = qkv(h, w_qkv, cos, sin)
            o, lse = attend(q, k, v_)
            if n < layers - 1:
                mid, after = post(h, o, w_od, w_gu)
            else:
                mid, after = h, None
            kept.append((h, q, k, v_, o, lse, mid))
            h = after
        mine, above = [None] * layers, None
        for n in reversed(range(layers)):
            w_qkv, w_od, w_gu = whole[n]
            h, q, k, v_, o, lse, mid = kept[n]
            by_mid, by_o, d_od, d_gu = post_bwd(mid, o, by, w_od, w_gu, n == layers - 1)
            if n < layers - 1:
                by_o, above = after_that(by_o, above)
                mine[n + 1] = (above, *mine[n + 1][1:])
            d_od, d_gu = scattered(d_od), scattered(d_gu)
            dq, dk, dv = attend_bwd(q, k, v_, by_o, o, lse)
            dq, d_od = after_that(dq, d_od)
            by, d_qkv = qkv_bwd(h, w_qkv, cos, sin, dq, dk, dv, by_mid if n else None)
            if n:
                by, d_gu = after_that(by, d_gu)
            else:
                d_qkv, d_gu = after_that(d_qkv, d_gu)
            above = scattered(d_qkv)
            mine[n] = above, d_od, d_gu
        d, ff, wide = x.shape[1], weights[4].shape[2], weights[0].shape[2]
        parts = []
        for d_qkv, d_od, d_gu in mine:
            parts.append((d_qkv[:, :wide], d_qkv[:, wide : wide + HEAD], d_qkv[:, wide + HEAD :], d_od[:, :d], d_gu[:, :ff], d_gu[:, ff:], d_od[:, d:]))
        new = []
        for i, (w, first, second) in enumerate(zip(weights, m, v, strict=True)):
            g = jnp.stack([part[i] for part in parts]).astype(F32)
            new.append(adamw(w.astype(F32), first, second, g))
        return tuple(one[which] for which in range(3) for one in new)

    states, cut = P(("rep", "dp"), None, None), P(None, "dp", None)
    return jax.shard_map(
        step,
        mesh=mesh,
        in_specs=(states, states) + (cut,) * 21,
        out_specs=(P("rep", "dp", None),) * 21,
        check_vma=False,
    )
```
